32 devices in a mesh: seq: 16 (over z, y, x), head: 2 (over core).
Axes of the slice: x: 2, y: 2, z: 4, core: 2. Of those that a mesh axis runs over, the one named last changes fastest.
Arguments:
- queries: bfloat16 [4096, 32, 128], P('seq', 'head'), may hold values from -192 to 192
- keys: bfloat16 [4096, 8, 128], P(('seq', 'head')), may hold values from -6 to 6
- values: bfloat16 [4096, 8, 128], P(('seq', 'head')), may hold values from -6 to 6
- doc_start: int32 [4096], P('seq'), may hold values from 0 to 4095, as said below
- tile_list: int32 [16, 18], P('seq'), may hold values from 0 to 31, as said below
- tile_count: int32 [16], P('seq'), may hold values from 2 to 18, as said below
Outputs:
- attention_out: bfloat16 [4096, 32, 128], P('seq', 'head')
The draws below stay inside these ranges and needn't reach their ends.
Inputs may be any that keep to these rules, and one draw needn't show every extreme that they name: doc_start never falls, doc_start[i] <= i, and a new document begins at each position where it changes; documents hold 1 to 2048 tokens, one exactly 2048. `tile_list`: row s holds in its first tile_count[s] entries, ascending, exactly the tiles (tile t holds key positions t * 128 to t * 128 + 127) that contain a key visible to some query of positions s * 256 to s * 256 + 255; the later entries equal s * 2. `tile_count`: some row reaches 18.
All inputs are finite; a program needn't handle non-finite values.
Results may differ from the reference program's by a relative error of at most 0.004.
Values may be sent and summed in bfloat16 or wider, within the bound.
No kernel may reach another device: no remote copies, remote signals or barrier semaphores. Data moves between devices by JAX's collectives and lax.ppermute only.
A program may use at most 64 MiB of HBM per device.

```python
import jax
import jax.numpy as jnp
from jax import lax

HQ = 32
KVH = 8
HD = 128
TOK_DEV = 256
TILE = 128
MAXDOC = 2048
REACH = 8
MAXT = 18
TOKENS = 4096
N_SEQ = 16


def document_starts(key):
    base_key = jax.random.fold_in(key, 11)
    choose_long = jax.random.randint(jax.random.fold_in(base_key, 1), (TOKENS,), 0, 2)
    short_len = jax.random.randint(jax.random.fold_in(base_key, 2), (TOKENS,), 1, TILE + 1)
    long_len = jax.random.randint(jax.random.fold_in(base_key, 3), (TOKENS,), TILE + 1, MAXDOC + 1)
    lengths = jnp.where(choose_long == 0, short_len, long_len).astype(jnp.int32)
    doc_ends = jnp.cumsum(lengths).astype(jnp.int32)
    start_marks = jnp.zeros((TOKENS,), jnp.int32).at[doc_ends].set(1, mode='drop')
    start_marks = start_marks.at[0].set(1)
    chosen = jax.random.randint(jax.random.fold_in(base_key, 4), (), REACH, N_SEQ).astype(jnp.int32)
    first_pos = chosen * TOK_DEV - MAXDOC + 1
    after_pos = chosen * TOK_DEV + 1
    position = jnp.arange(TOKENS, dtype=jnp.int32)
    inside = (position > first_pos) & (position < after_pos)
    start_marks = jnp.where(inside, 0, start_marks)
    start_marks = jnp.where((position == first_pos) | (position == after_pos), 1, start_marks)
    return lax.cummax(jnp.where(start_marks == 1, position, 0), axis=0).astype(jnp.int32)


def tile_tables(key):
    starts = document_starts(key)
    tiles_own = TOK_DEV // TILE
    first_tile = (starts[::TOK_DEV] // TILE).astype(jnp.int32)
    own_first = jnp.arange(N_SEQ, dtype=jnp.int32) * tiles_own
    slot_ids = jnp.arange(MAXT, dtype=jnp.int32)
    live_count = own_first + tiles_own - first_tile
    listed = first_tile[:, None] + slot_ids[None, :]
    listed = jnp.where(slot_ids[None, :] < live_count[:, None], listed, own_first[:, None])
    return (listed.astype(jnp.int32), live_count.astype(jnp.int32))


def attention_draws(key):
    base_key = jax.random.fold_in(key, 23)
    keys_raw = jax.random.truncated_normal(jax.random.fold_in(base_key, 1), -6.0, 6.0, (TOKENS, KVH, HD), jnp.float32)
    queries_raw = jax.random.truncated_normal(jax.random.fold_in(base_key, 2), -6.0, 6.0, (TOKENS, HQ, HD), jnp.float32)
    return (queries_raw, keys_raw)


def draw_queries(key, part):
    return attention_draws(key)[0].astype(jnp.bfloat16)


def draw_keys(key, part):
    return attention_draws(key)[1].astype(jnp.bfloat16)


def draw_doc_start(key, part):
    return document_starts(key)


def draw_tile_list(key, part):
    return tile_tables(key)[0]


def draw_tile_count(key, part):
    return tile_tables(key)[1]


def block_levels(rng, dims, cuts, low, high):
    level, own = 1.0, jax.random.fold_in(rng, 6)
    for dim, shards_of in cuts:
        draws = jnp.exp(jax.random.uniform(jax.random.fold_in(own, dim), (shards_of,), jnp.float32, low / len(cuts), high / len(cuts)))
        level = level * jnp.repeat(draws, dims[dim] // shards_of).reshape([-1 if axis == dim else 1 for axis in range(len(dims))])
    return level


def noise(own_key, shape, spread, reach, split=(), held_as=jnp.bfloat16):
    array = jax.random.normal(own_key, shape, jnp.float32) * spread
    if len(split) > 0:
        array = block_levels(own_key, shape, split, -0.22, 0.18) * array
    return jnp.clip(array, min=-reach, max=reach).astype(held_as)


def setup_inputs(seed: int = 0) -> dict:
    splits = jax.random.split(jax.random.key(seed), 7)
    queries = draw_queries(jax.random.fold_in(splits[6], 71), 0)
    keys = draw_keys(jax.random.fold_in(splits[6], 71), 0)
    values = noise(splits[2], (TOKENS, KVH, HD), 1.0, 6.0, ((0, 32),))
    doc_start = draw_doc_start(jax.random.fold_in(splits[6], 71), 0)
    tile_list = draw_tile_list(jax.random.fold_in(splits[6], 71), 0)
    tile_count = draw_tile_count(jax.random.fold_in(splits[6], 71), 0)
    return dict(queries=queries, keys=keys, values=values, doc_start=doc_start, tile_list=tile_list, tile_count=tile_count)


def reference(queries, keys, values, doc_start, tile_list, tile_count):
    group_size = HQ // KVH
    score_scale = 1.0 / (HD ** 0.5)
    key_tiles = keys.reshape(TOKENS // TILE, TILE, KVH, HD)
    value_tiles = values.reshape(TOKENS // TILE, TILE, KVH, HD)

    def one_shard(shard_index):
        query_block = lax.dynamic_slice_in_dim(queries, (shard_index * TOK_DEV).astype(jnp.int32), TOK_DEV, 0)
        starts = lax.dynamic_slice_in_dim(doc_start, (shard_index * TOK_DEV).astype(jnp.int32), TOK_DEV, 0)
        listed = tile_list[shard_index]
        live_count = tile_count[shard_index]
        key_block = key_tiles[listed].reshape(MAXT * TILE, KVH, HD)
        value_block = value_tiles[listed].reshape(MAXT * TILE, KVH, HD)
        key_pos = (listed[:, None] * TILE + jnp.arange(TILE, dtype=jnp.int32)[None, :]).reshape(-1)
        live_slot = jnp.repeat(jnp.arange(MAXT, dtype=jnp.int32) < live_count, TILE)
        query_pos = (shard_index * TOK_DEV).astype(jnp.int32) + jnp.arange(TOK_DEV, dtype=jnp.int32)
        visible = (key_pos[None, :] >= starts[:, None]) & (key_pos[None, :] <= query_pos[:, None]) & live_slot[None, :]
        grouped = query_block.reshape(TOK_DEV, KVH, group_size, HD).astype(jnp.float32)
        scores = jnp.einsum("tgch,kgh->gctk", grouped, key_block.astype(jnp.float32)) * score_scale
        scores = jnp.where(visible[None, None], scores, -jnp.inf)
        row_top = jnp.max(scores, axis=-1, keepdims=True)
        weights = jnp.where(visible[None, None], jnp.exp(scores - row_top), jnp.float32(0.0))
        weight_sum = jnp.sum(weights, axis=-1)
        rounded = lax.optimization_barrier(weights.astype(jnp.bfloat16)).astype(jnp.float32)
        summed = jnp.einsum("gctk,kgh->gcth", rounded, value_block.astype(jnp.float32))
        result = summed / weight_sum[..., None]
        result = jnp.transpose(result, (2, 0, 1, 3)).reshape(TOK_DEV, HQ, HD)
        return result.astype(jnp.bfloat16)

    blocks = lax.map(one_shard, jnp.arange(N_SEQ, dtype=jnp.int32))
    return blocks.reshape(TOKENS, HQ, HD)
```

```python
import functools

import jax
import jax.numpy as jnp
import numpy as np
from jax import lax
from jax.experimental import pallas as pl
from jax.experimental.pallas import tpu as pltpu
from jax.sharding import PartitionSpec as P

TILE = 128
MAXDOC = 2048
LOG2E = 1.4426950408889634
big_negative = -1e30


def attend_kernel(meta, *refs, blocks, first, last, factor, split):
    refs = list(refs)
    q_ref, starts_ref, pos_ref = refs[:3]
    block_refs = refs[3 : 3 + blocks]
    refs = refs[3 + blocks :]
    if not first:
        top_in, sum_in, acc_in = refs[:3]
        refs = refs[3:]
    if last:
        out_ref, top_ref, sum_ref, acc_ref, bias_ref = refs
    else:
        top_ref, sum_ref, acc_ref, bias_ref = refs
    group = q_ref.shape[0]
    tokens = q_ref.shape[1]
    tile = block_refs[0].shape[3]
    width = block_refs[0].shape[0] * tile

    if first:
        top_ref[...] = jnp.full(top_ref.shape, big_negative, jnp.float32)
        sum_ref[...] = jnp.zeros(sum_ref.shape, jnp.float32)
        acc_ref[...] = jnp.zeros(acc_ref.shape, jnp.float32)
    else:
        top_ref[...] = top_in[...]
        sum_ref[...] = sum_in[...]
        acc_ref[...] = acc_in[...]

    for b in range(blocks):
        base = meta[b, 0]
        live0 = meta[b, 1]
        live1 = meta[b, 2]

        @pl.when(live0 + live1 > 0)
        def _(b=b, base=base, live0=live0, live1=live1):
            blk = block_refs[b]

            @pl.when(pl.program_id(0) == 0)
            def _():
                row = lax.broadcasted_iota(jnp.int32, (width, tokens), 0)
                key_pos = row + base
                alive = jnp.where(row < tile, live0, live1) > 0
                seen = (key_pos >= starts_ref[...]) & (key_pos <= pos_ref[...]) & alive
                bias_ref[b] = jnp.where(seen, 0.0, big_negative)

            k = jnp.concatenate([blk[0, 0, 0], blk[1, 0, 0]], axis=0)
            v_t = jnp.concatenate([blk[0, 1, 0], blk[1, 1, 0]], axis=1)
            bias = bias_ref[b]
            for h in range(group):
                s = lax.dot_general(
                    k, q_ref[h], (((1,), (1,)), ((), ())), preferred_element_type=jnp.float32
                )
                s = s + bias
                top_old = top_ref[0, h : h + 1]
                top_new = jnp.maximum(top_old, jnp.max(s, axis=0, keepdims=True))
                p = jnp.exp2((s - top_new) * factor)
                alpha = jnp.exp2((top_old - top_new) * factor)
                top_ref[0, h : h + 1] = top_new
                part = jnp.sum(p.reshape(width // 8, 8, tokens), axis=0)
                sum_ref[0, h] = sum_ref[0, h] * alpha + part
                acc_ref[h] = acc_ref[h] * alpha + jnp.dot(
                    v_t, p.astype(jnp.bfloat16), preferred_element_type=jnp.float32
                )

    if last:
        for h in range(group):
            total = jnp.sum(sum_ref[0, h], axis=0, keepdims=True)
            out_ref[h] = (acc_ref[h] / total).T.astype(jnp.bfloat16)


def attend(q, starts, pos, meta, blocks, state, last):
    heads, tokens, head_dim = q.shape
    key_heads = blocks[0].shape[2]
    group = heads // key_heads
    first = state is None
    n = len(blocks)
    width = blocks[0].shape[0] * blocks[0].shape[3]
    q_spec = pl.BlockSpec((group, tokens, head_dim), lambda g, m: (g, 0, 0))
    row_spec = pl.BlockSpec((1, tokens), lambda g, m: (0, 0))
    bs = blocks[0].shape
    blk_spec = pl.BlockSpec((bs[0], bs[1], 1, bs[3], bs[4]), lambda g, m: (0, 0, g, 0, 0))
    top_spec = pl.BlockSpec((1, group, tokens), lambda g, m: (g, 0, 0))
    sum_spec = pl.BlockSpec((1, group, 8, tokens), lambda g, m: (g, 0, 0, 0))
    acc_spec = pl.BlockSpec((group, head_dim, tokens), lambda g, m: (g, 0, 0))
    state_specs = [top_spec, sum_spec, acc_spec]
    state_shapes = [
        jax.ShapeDtypeStruct((key_heads, group, tokens), jnp.float32),
        jax.ShapeDtypeStruct((key_heads, group, 8, tokens), jnp.float32),
        jax.ShapeDtypeStruct((heads, head_dim, tokens), jnp.float32),
    ]
    scratch = [pltpu.VMEM((n, width, tokens), jnp.float32)]
    if last:
        out_specs = q_spec
        out_shape = jax.ShapeDtypeStruct((heads, tokens, head_dim), jnp.bfloat16)
        scratch = [
            pltpu.VMEM((1, group, tokens), jnp.float32),
            pltpu.VMEM((1, group, 8, tokens), jnp.float32),
            pltpu.VMEM((group, head_dim, tokens), jnp.float32),
        ] + scratch
    else:
        out_specs, out_shape = state_specs, state_shapes
    kernel = functools.partial(
        attend_kernel,
        blocks=n,
        first=first,
        last=last,
        factor=float(head_dim ** (-0.5) * LOG2E),
        split=0,
    )
    call = pl.pallas_call(
        kernel,
        grid_spec=pltpu.PrefetchScalarGridSpec(
            num_scalar_prefetch=1,
            grid=(key_heads,),
            in_specs=[q_spec, row_spec, row_spec] + [blk_spec] * n + ([] if first else state_specs),
            out_specs=out_specs,
            scratch_shapes=scratch,
        ),
        out_shape=out_shape,
        cost_estimate=pl.CostEstimate(
            flops=4 * n * heads * tokens * width * head_dim, transcendentals=0, bytes_accessed=0
        ),
    )
    return call(meta, q, starts, pos, *blocks, *([] if first else state))


def permuted(x, pairs):
    return lax.ppermute(x, "seq", pairs)


def body(queries, keys, values, doc_start, tile_list, tile_count):
    tokens, query_heads, head_dim = queries.shape
    halves = lax.axis_size("head")
    devices = lax.axis_size("seq")
    key_heads = keys.shape[1] // halves
    own_tokens = keys.shape[0]
    tiles_own = tokens // TILE
    reach_back = MAXDOC // tokens
    side = reach_back // 2
    assert side == 4 and own_tokens == TILE and halves == tiles_own

    k = jnp.transpose(keys, (1, 0, 2)).reshape(halves, key_heads, TILE, head_dim)
    v = jnp.transpose(values, (1, 2, 0)).reshape(halves, key_heads, head_dim, TILE)
    own = lax.all_to_all(jnp.stack([k, v], 1), "head", split_axis=0, concat_axis=0, tiled=True)

    shard = lax.axis_index("seq")
    j = shard % side
    everyone = range(devices)
    ring = {0: 1, 1: 3, 3: 2, 2: 0}
    back = {b: a for a, b in ring.items()}

    def to(step, keep):
        return [(i, i - i % side + step(i % side)) for i in everyone if keep(i % side)]

    onward = [(i, i + side) for i in range(devices - side)]
    z1 = permuted(own, onward)
    up_x = permuted(own, to(lambda c: c ^ 1, lambda c: c < c ^ 1))
    up_y = permuted(own, to(lambda c: c ^ 2, lambda c: c < c ^ 2))
    z2 = permuted(z1, onward)
    x1 = permuted(z1, to(lambda c: c ^ 1, lambda c: True))
    y1 = permuted(z1, to(lambda c: c ^ 2, lambda c: True))
    relay0 = permuted(
        jnp.where(j == 1, up_x, up_y), to(lambda c: ring[c], lambda c: c in (1, 3))
    )
    relay1 = permuted(
        jnp.where((j == 0) | (j == 3), x1, y1), to(lambda c: back[c], lambda c: True)
    )
    down_x = permuted(z2, to(lambda c: c ^ 1, lambda c: c > c ^ 1))
    down_y = permuted(z2, to(lambda c: c ^ 2, lambda c: c > c ^ 2))
    relay2 = permuted(
        jnp.where(j == 0, down_y, down_x), to(lambda c: ring[c], lambda c: c in (0, 2))
    )

    slot_live = jnp.arange(tile_list.shape[1], dtype=jnp.int32) < tile_count[0]
    listed = jnp.where(slot_live, tile_list[0], -1)

    never = jnp.int32(-1)
    one = shard - side
    two = shard - 2 * side
    diagonal = lambda plane: plane - j + (side - 1 - j)
    beside = lambda plane, bit: plane - j + (j ^ bit)
    ids = [
        shard,
        one,
        jnp.where(j > (j ^ 1), beside(shard, 1), never),
        jnp.where(j > (j ^ 2), beside(shard, 2), never),
        two,
        beside(one, 1),
        beside(one, 2),
        jnp.where(j >= 2, diagonal(shard), never),
        diagonal(one),
        jnp.where(j < (j ^ 1), beside(two, 1), never),
        jnp.where(j < (j ^ 2), beside(two, 2), never),
        jnp.where(j < 2, diagonal(two), never),
    ]
    ids = jnp.stack(ids)
    tiles = ids[:, None] * tiles_own + jnp.arange(tiles_own, dtype=jnp.int32)[None, :]
    live = jnp.any(tiles[:, :, None] == listed[None, None, :], axis=2) & (ids[:, None] >= 0)
    meta = jnp.concatenate([ids[:, None] * tokens, live.astype(jnp.int32)], axis=1)

    q = jnp.transpose(queries, (1, 0, 2))
    starts = doc_start.reshape(1, tokens)
    pos = (shard * tokens + jnp.arange(tokens, dtype=jnp.int32)).reshape(1, tokens)
    groups = [
        [own, z1, up_x, up_y],
        [z2, x1, y1, relay0],
        [relay1, down_x, down_y, relay2],
    ]
    state = None
    at = 0
    for n, blocks in enumerate(groups):
        state = attend(
            q, starts, pos, meta[at : at + len(blocks)], blocks, state, n == len(groups) - 1
        )
        at += len(blocks)
    return jnp.transpose(state, (1, 0, 2))


def solution(mesh):
    in_specs = (
        P("seq", "head", None),
        P(("seq", "head"), None, None),
        P(("seq", "head"), None, None),
        P("seq"),
        P("seq", None),
        P("seq"),
    )
    out_specs = P("seq", "head", None)
    return jax.shard_map(body, mesh=mesh, in_specs=in_specs, out_specs=out_specs, check_vma=False)
```

```python
import functools

import jax
import jax.numpy as jnp
from jax import lax
from jax.experimental import pallas as pl
from jax.experimental.pallas import tpu as pltpu
from jax.sharding import PartitionSpec as P


TILE = 128
MAXDOC = 2048
LOG2E = 1.4426950408889634
big_negative = -1e30


def attend_kernel(meta, *refs, blocks, first, last, factor):
    refs = list(refs)
    q_ref, starts_ref, pos_ref = refs[:3]
    block_refs = refs[3 : 3 + blocks]
    refs = refs[3 + blocks :]
    if not first:
        top_in, sum_in, acc_in = refs[:3]
        refs = refs[3:]
    if last:
        out_ref, top_ref, sum_ref, acc_ref, bias_ref = refs
    else:
        top_ref, sum_ref, acc_ref, bias_ref = refs
    group = q_ref.shape[0]
    tokens = q_ref.shape[1]
    tile = block_refs[0].shape[3]
    width = block_refs[0].shape[0] * tile

    if first:
        top_ref[...] = jnp.full(top_ref.shape, big_negative, jnp.float32)
        sum_ref[...] = jnp.zeros(sum_ref.shape, jnp.float32)
        acc_ref[...] = jnp.zeros(acc_ref.shape, jnp.float32)
    else:
        top_ref[...] = top_in[...]
        sum_ref[...] = sum_in[...]
        acc_ref[...] = acc_in[...]

    @pl.when(pl.program_id(0) == 0)
    def _():
        row = lax.broadcasted_iota(jnp.int32, (width, tokens), 0)
        for b in range(blocks):
            key_pos = row + meta[b, 0]
            alive = jnp.where(row < tile, meta[b, 1], meta[b, 2]) > 0
            seen = (key_pos >= starts_ref[...]) & (key_pos <= pos_ref[...]) & alive
            bias_ref[b] = jnp.where(seen, 0.0, big_negative)

    for h in range(group):
        q = q_ref[h]
        top_old = top_ref[0, h : h + 1]
        scores = []
        top_new = top_old
        for blk in block_refs:
            k = blk[:, 0, 0].reshape(width, q.shape[1])
            s = lax.dot_general(
                k, q, (((1,), (1,)), ((), ())), preferred_element_type=jnp.float32
            )
            s = s + bias_ref[len(scores)]
            scores.append(s)
            top_new = jnp.maximum(top_new, jnp.max(s, axis=0, keepdims=True))
        alpha = jnp.exp2((top_old - top_new) * factor)
        top_ref[0, h : h + 1] = top_new
        weight_sum = sum_ref[0, h] * alpha
        acc = acc_ref[h] * alpha
        for blk, s in zip(block_refs, scores):
            p = jnp.exp2((s - top_new) * factor)
            weight_sum = weight_sum + jnp.sum(p.reshape(width // 8, 8, tokens), axis=0)
            v_t = jnp.concatenate([blk[0, 1, 0], blk[1, 1, 0]], axis=1)
            acc = acc + jnp.dot(v_t, p.astype(jnp.bfloat16), preferred_element_type=jnp.float32)
        sum_ref[0, h] = weight_sum
        acc_ref[h] = acc

    if last:
        for h in range(group):
            total = jnp.sum(sum_ref[0, h], axis=0, keepdims=True)
            out_ref[h] = (acc_ref[h] / total).T.astype(jnp.bfloat16)


def attend(q, starts, pos, meta, blocks, state, last):
    heads, tokens, head_dim = q.shape
    key_heads = blocks[0].shape[2]
    group = heads // key_heads
    first = state is None
    n = len(blocks)
    width = blocks[0].shape[0] * blocks[0].shape[3]
    q_spec = pl.BlockSpec((group, tokens, head_dim), lambda g, m: (g, 0, 0))
    row_spec = pl.BlockSpec((1, tokens), lambda g, m: (0, 0))
    bs = blocks[0].shape
    blk_spec = pl.BlockSpec((bs[0], bs[1], 1, bs[3], bs[4]), lambda g, m: (0, 0, g, 0, 0))
    top_spec = pl.BlockSpec((1, group, tokens), lambda g, m: (g, 0, 0))
    sum_spec = pl.BlockSpec((1, group, 8, tokens), lambda g, m: (g, 0, 0, 0))
    acc_spec = pl.BlockSpec((group, head_dim, tokens), lambda g, m: (g, 0, 0))
    state_specs = [top_spec, sum_spec, acc_spec]
    state_shapes = [
        jax.ShapeDtypeStruct((key_heads, group, tokens), jnp.float32),
        jax.ShapeDtypeStruct((key_heads, group, 8, tokens), jnp.float32),
        jax.ShapeDtypeStruct((heads, head_dim, tokens), jnp.float32),
    ]
    scratch = [pltpu.VMEM((n, width, tokens), jnp.float32)]
    if last:
        out_specs = q_spec
        out_shape = jax.ShapeDtypeStruct((heads, tokens, head_dim), jnp.bfloat16)
        scratch = [
            pltpu.VMEM((1, group, tokens), jnp.float32),
            pltpu.VMEM((1, group, 8, tokens), jnp.float32),
            pltpu.VMEM((group, head_dim, tokens), jnp.float32),
        ] + scratch
    else:
        out_specs, out_shape = state_specs, state_shapes
    kernel = functools.partial(
        attend_kernel, blocks=n, first=first, last=last, factor=float(head_dim ** (-0.5) * LOG2E)
    )
    call = pl.pallas_call(
        kernel,
        grid_spec=pltpu.PrefetchScalarGridSpec(
            num_scalar_prefetch=1,
            grid=(key_heads,),
            in_specs=[q_spec, row_spec, row_spec] + [blk_spec] * n + ([] if first else state_specs),
            out_specs=out_specs,
            scratch_shapes=scratch,
        ),
        out_shape=out_shape,
        cost_estimate=pl.CostEstimate(
            flops=4 * n * heads * tokens * width * head_dim, transcendentals=0, bytes_accessed=0
        ),
    )
    return call(meta, q, starts, pos, *blocks, *([] if first else state))


def permuted(x, pairs):
    return lax.ppermute(x, "seq", pairs)


def body(queries, keys, values, doc_start, tile_list, tile_count):
    tokens, _, head_dim = queries.shape
    halves = lax.axis_size("head")
    devices = lax.axis_size("seq")
    key_heads = keys.shape[1] // halves
    own_tokens = keys.shape[0]
    tiles_own = tokens // TILE
    reach_back = MAXDOC // tokens
    side = reach_back // 2
    assert side == 4 and own_tokens == TILE and halves == tiles_own

    k = jnp.transpose(keys, (1, 0, 2)).reshape(halves, key_heads, TILE, head_dim)
    v = jnp.transpose(values, (1, 2, 0)).reshape(halves, key_heads, head_dim, TILE)
    own = lax.all_to_all(jnp.stack([k, v], 1), "head", split_axis=0, concat_axis=0, tiled=True)

    shard = lax.axis_index("seq")
    j = shard % side
    everyone = range(devices)
    ring = {0: 1, 1: 3, 3: 2, 2: 0}
    back = {b: a for a, b in ring.items()}

    def to(step, keep):
        return [(i, i - i % side + step(i % side)) for i in everyone if keep(i % side)]

    onward = [(i, i + side) for i in range(devices - side)]
    z1 = permuted(own, onward)
    up_x = permuted(own, to(lambda c: c ^ 1, lambda c: c < c ^ 1))
    up_y = permuted(own, to(lambda c: c ^ 2, lambda c: c < c ^ 2))
    z2 = permuted(z1, onward)
    x1 = permuted(z1, to(lambda c: c ^ 1, lambda c: True))
    y1 = permuted(z1, to(lambda c: c ^ 2, lambda c: True))
    relay0 = permuted(jnp.where(j == 1, up_x, up_y), to(lambda c: ring[c], lambda c: c in (1, 3)))
    relay1 = permuted(jnp.where((j == 0) | (j == 3), x1, y1), to(lambda c: back[c], lambda c: True))
    down_x = permuted(z2, to(lambda c: c ^ 1, lambda c: c > c ^ 1))
    down_y = permuted(z2, to(lambda c: c ^ 2, lambda c: c > c ^ 2))
    relay2 = permuted(
        jnp.where(j == 0, down_y, down_x), to(lambda c: ring[c], lambda c: c in (0, 2))
    )

    slot_live = jnp.arange(tile_list.shape[1], dtype=jnp.int32) < tile_count[0]
    listed = jnp.where(slot_live, tile_list[0], -1)

    never = jnp.int32(-1)
    one = shard - side
    two = shard - 2 * side
    diagonal = lambda plane: plane - j + (side - 1 - j)
    beside = lambda plane, bit: plane - j + (j ^ bit)
    ids = [
        shard,
        one,
        jnp.where(j > (j ^ 1), beside(shard, 1), never),
        jnp.where(j > (j ^ 2), beside(shard, 2), never),
        two,
        beside(one, 1),
        beside(one, 2),
        jnp.where(j >= 2, diagonal(shard), never),
        diagonal(one),
        jnp.where(j < (j ^ 1), beside(two, 1), never),
        jnp.where(j < (j ^ 2), beside(two, 2), never),
        jnp.where(j < 2, diagonal(two), never),
    ]
    ids = jnp.stack(ids)
    tiles = ids[:, None] * tiles_own + jnp.arange(tiles_own, dtype=jnp.int32)[None, :]
    live = jnp.any(tiles[:, :, None] == listed[None, None, :], axis=2) & (ids[:, None] >= 0)
    meta = jnp.concatenate([ids[:, None] * tokens, live.astype(jnp.int32)], axis=1)

    q = jnp.transpose(queries, (1, 0, 2))
    starts = doc_start.reshape(1, tokens)
    pos = (shard * tokens + jnp.arange(tokens, dtype=jnp.int32)).reshape(1, tokens)
    groups = [
        [own, z1, up_x, up_y],
        [z2, x1, y1, relay0],
        [relay1, down_x, down_y, relay2],
    ]
    state = None
    at = 0
    for n, blocks in enumerate(groups):
        state = attend(
            q, starts, pos, meta[at : at + len(blocks)], blocks, state, n == len(groups) - 1
        )
        at += len(blocks)
    return jnp.transpose(state, (1, 0, 2))


def solution(mesh):
    in_specs = (
        P("seq", "head", None),
        P(("seq", "head"), None, None),
        P(("seq", "head"), None, None),
        P("seq"),
        P("seq", None),
        P("seq"),
    )
    out_specs = P("seq", "head", None)
    return jax.shard_map(body, mesh=mesh, in_specs=in_specs, out_specs=out_specs, check_vma=False)
```

```python
import functools

import jax
import jax.numpy as jnp
from jax import lax
from jax.experimental import pallas as pl
from jax.experimental.pallas import tpu as pltpu
from jax.sharding import PartitionSpec as P


TILE = 128
MAXDOC = 2048
LOG2E = 1.4426950408889634
big_negative = -1e30


def attend_kernel(meta, *refs, blocks, first, last, factor, at):
    refs = list(refs)
    q_ref, starts_ref, pos_ref = refs[:3]
    block_refs = refs[3 : 3 + blocks]
    refs = refs[3 + blocks :]
    if not first:
        top_in, sum_in, acc_in = refs[:3]
        refs = refs[3:]
    if last:
        out_ref, top_ref, sum_ref, acc_ref, bias_ref = refs
    else:
        top_ref, sum_ref, acc_ref, bias_ref = refs
    group = q_ref.shape[0]
    tokens = q_ref.shape[1]
    tile = block_refs[0].shape[3]
    width = block_refs[0].shape[0] * tile

    if first:
        top_ref[...] = jnp.full(top_ref.shape, big_negative, jnp.float32)
        sum_ref[...] = jnp.zeros(sum_ref.shape, jnp.float32)
        acc_ref[...] = jnp.zeros(acc_ref.shape, jnp.float32)
    else:
        top_ref[...] = top_in[...]
        sum_ref[...] = sum_in[...]
        acc_ref[...] = acc_in[...]

    @pl.when(pl.program_id(0) == 0)
    def _():
        row = lax.broadcasted_iota(jnp.int32, (width, tokens), 0)
        for b in range(blocks):
            key_pos = row + meta[at + b, 0]
            alive = jnp.where(row < tile, meta[at + b, 1], meta[at + b, 2]) > 0
            seen = (key_pos >= starts_ref[...]) & (key_pos <= pos_ref[...]) & alive
            bias_ref[b] = jnp.where(seen, 0.0, big_negative)

    for h in range(group):
        q = q_ref[h]
        top_old = top_ref[0, h : h + 1]
        scores = []
        top_new = top_old
        for blk in block_refs:
            k = blk[:, 0, 0].reshape(width, q.shape[1])
            s = lax.dot_general(
                k, q, (((1,), (1,)), ((), ())), preferred_element_type=jnp.float32
            )
            s = s + bias_ref[len(scores)]
            scores.append(s)
            top_new = jnp.maximum(top_new, jnp.max(s, axis=0, keepdims=True))
        alpha = jnp.exp2((top_old - top_new) * factor)
        top_ref[0, h : h + 1] = top_new
        weight_sum = sum_ref[0, h] * alpha
        acc = acc_ref[h] * alpha
        for blk, s in zip(block_refs, scores):
            p = jnp.exp2((s - top_new) * factor)
            weight_sum = weight_sum + jnp.sum(p.reshape(width // 8, 8, tokens), axis=0)
            v_t = jnp.concatenate([blk[0, 1, 0], blk[1, 1, 0]], axis=1)
            acc = acc + jnp.dot(v_t, p.astype(jnp.bfloat16), preferred_element_type=jnp.float32)
        sum_ref[0, h] = weight_sum
        acc_ref[h] = acc

    if last:
        for h in range(group):
            total = jnp.sum(sum_ref[0, h], axis=0, keepdims=True)
            out_ref[h] = (acc_ref[h] / total).T.astype(jnp.bfloat16)


def attend(q, starts, pos, meta, blocks, state, last, at=0):
    heads, tokens, head_dim = q.shape
    key_heads = blocks[0].shape[2]
    group = heads // key_heads
    first = state is None
    n = len(blocks)
    width = blocks[0].shape[0] * blocks[0].shape[3]
    q_spec = pl.BlockSpec((group, tokens, head_dim), lambda g, m: (g, 0, 0))
    row_spec = pl.BlockSpec((1, tokens), lambda g, m: (0, 0))
    bs = blocks[0].shape
    blk_spec = pl.BlockSpec((bs[0], bs[1], 1, bs[3], bs[4]), lambda g, m: (0, 0, g, 0, 0))
    top_spec = pl.BlockSpec((1, group, tokens), lambda g, m: (g, 0, 0))
    sum_spec = pl.BlockSpec((1, group, 8, tokens), lambda g, m: (g, 0, 0, 0))
    acc_spec = pl.BlockSpec((group, head_dim, tokens), lambda g, m: (g, 0, 0))
    state_specs = [top_spec, sum_spec, acc_spec]
    state_shapes = [
        jax.ShapeDtypeStruct((key_heads, group, tokens), jnp.float32),
        jax.ShapeDtypeStruct((key_heads, group, 8, tokens), jnp.float32),
        jax.ShapeDtypeStruct((heads, head_dim, tokens), jnp.float32),
    ]
    scratch = [pltpu.VMEM((n, width, tokens), jnp.float32)]
    if last:
        out_specs = q_spec
        out_shape = jax.ShapeDtypeStruct((heads, tokens, head_dim), jnp.bfloat16)
        scratch = [
            pltpu.VMEM((1, group, tokens), jnp.float32),
            pltpu.VMEM((1, group, 8, tokens), jnp.float32),
            pltpu.VMEM((group, head_dim, tokens), jnp.float32),
        ] + scratch
    else:
        out_specs, out_shape = state_specs, state_shapes
    kernel = functools.partial(
        attend_kernel,
        blocks=n,
        first=first,
        last=last,
        factor=float(head_dim ** (-0.5) * LOG2E),
        at=at,
    )
    call = pl.pallas_call(
        kernel,
        grid_spec=pltpu.PrefetchScalarGridSpec(
            num_scalar_prefetch=1,
            grid=(key_heads,),
            in_specs=[q_spec, row_spec, row_spec] + [blk_spec] * n + ([] if first else state_specs),
            out_specs=out_specs,
            scratch_shapes=scratch,
        ),
        out_shape=out_shape,
        cost_estimate=pl.CostEstimate(
            flops=4 * n * heads * tokens * width * head_dim, transcendentals=0, bytes_accessed=0
        ),
    )
    return call(meta, q, starts, pos, *blocks, *([] if first else state))


def permuted(x, pairs):
    return lax.ppermute(x, "seq", pairs)


def body(queries, keys, values, doc_start, tile_list, tile_count):
    tokens, _, head_dim = queries.shape
    halves = lax.axis_size("head")
    devices = lax.axis_size("seq")
    key_heads = keys.shape[1] // halves
    own_tokens = keys.shape[0]
    tiles_own = tokens // TILE
    reach_back = MAXDOC // tokens
    side = reach_back // 2
    assert side == 4 and own_tokens == TILE and halves == tiles_own

    k = jnp.transpose(keys, (1, 0, 2)).reshape(halves, key_heads, TILE, head_dim)
    v = jnp.transpose(values, (1, 2, 0)).reshape(halves, key_heads, head_dim, TILE)
    own = lax.all_to_all(jnp.stack([k, v], 1), "head", split_axis=0, concat_axis=0, tiled=True)

    shard = lax.axis_index("seq")
    j = shard % side
    everyone = range(devices)
    ring = {0: 1, 1: 3, 3: 2, 2: 0}
    back = {b: a for a, b in ring.items()}

    def to(step, keep):
        return [(i, i - i % side + step(i % side)) for i in everyone if keep(i % side)]

    onward = [(i, i + side) for i in range(devices - side)]
    z1 = permuted(own, onward)
    up_x = permuted(own, to(lambda c: c ^ 1, lambda c: c < c ^ 1))
    up_y = permuted(own, to(lambda c: c ^ 2, lambda c: c < c ^ 2))
    z2 = permuted(z1, onward)
    x1 = permuted(z1, to(lambda c: c ^ 1, lambda c: True))
    y1 = permuted(z1, to(lambda c: c ^ 2, lambda c: True))
    relay0 = permuted(jnp.where(j == 1, up_x, up_y), to(lambda c: ring[c], lambda c: c in (1, 3)))
    relay1 = permuted(jnp.where((j == 0) | (j == 3), x1, y1), to(lambda c: back[c], lambda c: True))
    down_x = permuted(z2, to(lambda c: c ^ 1, lambda c: c > c ^ 1))
    down_y = permuted(z2, to(lambda c: c ^ 2, lambda c: c > c ^ 2))
    relay2 = permuted(
        jnp.where(j == 0, down_y, down_x), to(lambda c: ring[c], lambda c: c in (0, 2))
    )

    slot_live = jnp.arange(tile_list.shape[1], dtype=jnp.int32) < tile_count[0]
    listed = jnp.where(slot_live, tile_list[0], -1)

    never = jnp.int32(-1)
    one = shard - side
    two = shard - 2 * side
    diagonal = lambda plane: plane - j + (side - 1 - j)
    beside = lambda plane, bit: plane - j + (j ^ bit)
    ids = [
        shard,
        one,
        jnp.where(j > (j ^ 1), beside(shard, 1), never),
        jnp.where(j > (j ^ 2), beside(shard, 2), never),
        two,
        beside(one, 1),
        beside(one, 2),
        jnp.where(j >= 2, diagonal(shard), never),
        jnp.where(j < (j ^ 1), beside(two, 1), never),
        jnp.where(j < (j ^ 2), beside(two, 2), never),
        diagonal(one),
        jnp.where(j < 2, diagonal(two), never),
    ]
    ids = jnp.stack(ids)
    tiles = ids[:, None] * tiles_own + jnp.arange(tiles_own, dtype=jnp.int32)[None, :]
    live = jnp.any(tiles[:, :, None] == listed[None, None, :], axis=2) & (ids[:, None] >= 0)
    meta = jnp.concatenate([ids[:, None] * tokens, live.astype(jnp.int32)], axis=1)

    q = jnp.transpose(queries, (1, 0, 2))
    starts = doc_start.reshape(1, tokens)
    pos = (shard * tokens + jnp.arange(tokens, dtype=jnp.int32)).reshape(1, tokens)
    groups = [
        [own, z1, up_x, up_y],
        [z2, x1, y1, relay0, down_x, down_y],
        [relay1, relay2],
    ]
    state = None
    at = 0
    for n, blocks in enumerate(groups):
        state = attend(
            q, starts, pos, meta, blocks, state, n == len(groups) - 1, at
        )
        at += len(blocks)
    return jnp.transpose(state, (1, 0, 2))


def solution(mesh):
    in_specs = (
        P("seq", "head", None),
        P(("seq", "head"), None, None),
        P(("seq", "head"), None, None),
        P("seq"),
        P("seq", None),
        P("seq"),
    )
    out_specs = P("seq", "head", None)
    return jax.shard_map(body, mesh=mesh, in_specs=in_specs, out_specs=out_specs, check_vma=False)
```
